32 devices in a mesh: pair: 4 (over z), aux: 8 (over y, x, core).
Axes of the slice: x: 2, y: 2, z: 4, core: 2. Of those that a mesh axis runs over, the one named last changes fastest.
Arguments:
- integrals: bfloat16 [12288, 12288], P('pair', 'aux'), may hold values from -0.1875 to 0.1875
- energy_gaps: float32 [12288], P('pair'), may hold values from 0.3 to 3
- trial_vectors: float32 [12288, 64], P('pair'), may hold values from -160 to 160
Outputs:
- sigma_vectors: float32 [12288, 64], P(('pair', 'aux'))
- subspace: float32 [64, 64], replicated
- residuals: float32 [12288, 64], P(('pair', 'aux'))
- residual_norms: float32 [64], replicated
The draws below stay inside these ranges and needn't reach their ends.
All inputs are finite; a program needn't handle non-finite values.
Results may differ from the reference program's by a relative error of at most 0.0052.
Values may be sent and summed in bfloat16 or wider, within the bound.
A program may use at most 64 MiB of HBM per device.

```python
import math
import jax
import jax.numpy as jnp
from jax import lax

NAUX = 12288
NVEC = 64
PAIRS = 12288


def draw_trial_vectors(key, part):
    key_entries = jax.random.fold_in(key, 11)
    key_rows = jax.random.fold_in(key, 12)
    key_columns = jax.random.fold_in(key, 13)
    positions = jnp.arange(PAIRS).astype(jnp.float32)
    growth = jnp.exp(jnp.log(3.0) * positions / PAIRS)
    row_scale = jnp.exp(jax.random.uniform(key_rows, (PAIRS,), jnp.float32, jnp.log(0.3), jnp.log(3.0)))
    entries = jnp.clip(jax.random.normal(key_entries, (PAIRS, NVEC), jnp.float32), -5.0, 5.0)
    column_scale = jnp.exp(jax.random.uniform(key_columns, (NVEC,), jnp.float32, jnp.log(0.3), jnp.log(3.0)))
    return (entries * (growth * row_scale)[:, None] * column_scale[None, :]).astype(jnp.float32)


def spiked(values, rng, source, target, blocks, factor):
    def block_of(dim):
        return (jnp.arange(values.shape[dim]) // (values.shape[dim] // blocks)).reshape((-1,) + (1,) * (values.ndim - 1 - dim))

    first = jax.random.permutation(rng, blocks)[block_of(target)]
    second = (block_of(target) + blocks // 2) % blocks
    return jnp.where((block_of(source) == first) | (block_of(source) == second), factor * values, values)


def block_levels(rng, extent, split, low, high):
    factor_of, own = 1.0, jax.random.fold_in(rng, 6)
    for dim, blocks in split:
        heights = jnp.exp(jax.random.uniform(jax.random.fold_in(own, dim), (blocks,), jnp.float32, low / len(split), high / len(split)))
        factor_of = factor_of * jnp.repeat(heights, extent[dim] // blocks).reshape([-1 if axis == dim else 1 for axis in range(len(extent))])
    return factor_of


def heavy_noise(rng, shape, spread, limit, pieces, heavy, held_as=jnp.bfloat16):
    values = spread * jax.random.normal(rng, shape, jnp.float32)
    if pieces:
        values = values * block_levels(rng, shape, pieces, -0.22, 0.18)
    return jnp.clip(spiked(values, jax.random.fold_in(rng, 3), *heavy), -limit, limit).astype(held_as)


def setup_inputs(seed: int = 0) -> dict:
    streams_of = jax.random.split(jax.random.key(seed), 4)
    return {
        "integrals": heavy_noise(streams_of[0], (PAIRS, NAUX), (1.0 / (PAIRS * NAUX) ** 0.25), 0.1875, ((0, 4), (1, 8)), (0, 1, 8, 2.0)),
        "energy_gaps": jnp.clip(jnp.exp(math.log(3.0) - 2.3025851 * jax.random.uniform(streams_of[1], (PAIRS,), jnp.float32) ** block_levels(streams_of[1], (PAIRS,), ((0, 4),), -0.2, 0.2)), 0.3, 3.0),
        "trial_vectors": draw_trial_vectors(jax.random.fold_in(streams_of[3], 71), 0),
    }


epsilon = 1e-06

def reference(integrals, energy_gaps, trial_vectors):
    trial_half = trial_vectors.astype(jnp.bfloat16)
    aux_totals = lax.dot_general(integrals, trial_half, (((0,), (0,)), ((), ())), preferred_element_type=jnp.float32)
    aux_half = aux_totals.astype(jnp.bfloat16)
    coupled = jnp.dot(integrals, aux_half, preferred_element_type=jnp.float32)
    sigma_vectors = energy_gaps[:, None] * trial_vectors + 2.0 * coupled
    subspace = lax.dot_general(trial_vectors, sigma_vectors, (((0,), (0,)), ((), ())), precision=lax.Precision.HIGHEST, preferred_element_type=jnp.float32) / PAIRS
    intersection = lax.optimization_barrier(jnp.sum(trial_vectors * trial_vectors, axis=0)) / PAIRS
    rayleigh = jnp.diagonal(subspace) / (intersection + epsilon)
    residuals = sigma_vectors - trial_vectors * rayleigh[None, :]
    residual_norms = jnp.sqrt(lax.optimization_barrier(jnp.sum(residuals * residuals, axis=0)) / PAIRS + epsilon)
    return (sigma_vectors, subspace, residuals, residual_norms)
```

```python
import functools

import jax
import jax.numpy as jnp
from jax import lax
from jax.experimental import pallas as pl
from jax.experimental.pallas import tpu as pltpu
from jax.sharding import PartitionSpec as P

epsilon = 1e-06
MESH = pl.DeviceIdType.MESH
f32, bf16 = jnp.float32, jnp.bfloat16
WIDTH = 256
VMEM = 48 * 1024 * 1024
LAG = 3
NT = (((1,), (1,)), ((), ()))


def exact(a, b):
    return lax.dot_general(a, b, NT, precision=lax.Precision.HIGHEST, preferred_element_type=f32)


def kernel(
    np_, na, chunks, width, share,
    ints_hbm, gaps_hbm, trial_hbm,
    sigma, sub, res, norm,
    ints, gaps, trial, half, own, acc, mat, gram,
    pre_in, pre_out, suf_in, suf_out,
    b1_out, b1_in, b2_out, b2_in,
    m1_out, m1_in, m2, m3, n1, n2,
    load, aload, pre_s, pre_r, suf_s, suf_r,
    b1_s, b1_r, b2_s, b2_r, m1_s, m1_r, m2_s, m2_r, m3_s, m3_r, n1_s, n1_r, n2_s, n2_r,
):
    z, a = lax.axis_index("pair"), lax.axis_index("aux")
    core, chip, chips = a % 2, a // 2, na // 2
    vecs = trial.shape[0]

    trial_load = pltpu.make_async_copy(trial_hbm, trial, aload.at[0])
    gaps_load = pltpu.make_async_copy(gaps_hbm, gaps, aload.at[1])
    trial_load.start()
    loads = [
        pltpu.make_async_copy(ints_hbm.at[:, pl.ds(c * width, width)], ints.at[c], load.at[c])
        for c in range(chunks)
    ]
    loads[0].start()
    gaps_load.start()
    for c in range(1, chunks):
        loads[c].start()

    barrier = pltpu.get_barrier_semaphore()
    for d in range(1, np_):
        pl.semaphore_signal(barrier, inc=1, device_id={"pair": (z + d) % np_, "aux": a}, device_id_type=MESH)
    for d in range(1, na):
        pl.semaphore_signal(barrier, inc=1, device_id={"pair": z, "aux": (a + d) % na}, device_id_type=MESH)

    def remote(src, dst, s, r, pair, aux):
        return pltpu.make_async_remote_copy(
            src_ref=src, dst_ref=dst, send_sem=s, recv_sem=r,
            device_id={"pair": pair, "aux": aux}, device_id_type=MESH,
        )

    def prefix(c):
        return remote(pre_out.at[c], pre_in.at[c], pre_s.at[c], pre_r.at[c], z + 1, a)

    def suffix(c):
        return remote(suf_out.at[c], suf_in.at[c], suf_s.at[c], suf_r.at[c], z - 1, a)

    acc[...] = jnp.zeros_like(acc)
    mat[...] = jnp.zeros_like(mat)
    trial_load.wait()
    half[...] = trial[...].astype(bf16)
    gaps_load.wait()
    first = pl.multiple_of(a * share, 128)
    rows = share // 128

    def own_trial():
        return trial[:, pl.ds(first, share)]

    def own_gaps():
        return jnp.concatenate([gaps[pl.ds(a * rows + q, 1), :] for q in range(rows)], axis=1)

    eye = lax.broadcasted_iota(jnp.int32, (vecs, vecs), 0) == lax.broadcasted_iota(jnp.int32, (vecs, vecs), 1)

    def as_row(column):
        return jnp.sum(jnp.where(eye, column, 0.0), axis=0, keepdims=True)

    mine = own_trial()
    gram[...] = exact(mine, mine * own_gaps())
    pl.semaphore_wait(barrier, np_ - 1 + na - 1)

    after = np_ - 1 - z
    longest = jnp.maximum(z, after)

    def step(t, carry):
        @pl.when(t < chunks)
        def _():
            pltpu.make_async_copy(ints_hbm.at[:, pl.ds(0, width)], ints.at[t], load.at[t]).wait()
            own[t] = jnp.dot(half[...], ints[t], preferred_element_type=f32)

        p = t - LAG * z

        @pl.when((p >= 0) & (p < chunks) & (after > 0))
        def _():
            @pl.when(z == 0)
            def _():
                pre_out[p] = own[p].astype(bf16)

            @pl.when(z > 0)
            def _():
                prefix(p).wait_recv()
                pre_out[p] = (own[p] + pre_in[p].astype(f32)).astype(bf16)

            prefix(p).start()

        s = t - LAG * after

        @pl.when((s >= 0) & (s < chunks) & (z > 0))
        def _():
            @pl.when(after == 0)
            def _():
                suf_out[s] = own[s].astype(bf16)

            @pl.when(after > 0)
            def _():
                suffix(s).wait_recv()
                suf_out[s] = (own[s] + suf_in[s].astype(f32)).astype(bf16)

            suffix(s).start()

        c = t - LAG * longest

        @pl.when((c >= 0) & (c < chunks))
        def _():
            @pl.when(z == np_ - 1)
            def _():
                prefix(c).wait_recv()

            @pl.when(z == 0)
            def _():
                suffix(c).wait_recv()

            @pl.when(z > 0)
            def _():
                own[c] = own[c] + pre_in[c].astype(f32)

            @pl.when(after > 0)
            def _():
                own[c] = own[c] + suf_in[c].astype(f32)

            aux = own[c].astype(bf16)
            for b in range(chips):
                part = lax.dot_general(
                    aux, ints[c, pl.ds(b * 2 * share, 2 * share), :], NT, preferred_element_type=f32
                )
                acc[2 * b] += part[:, :share]
                acc[2 * b + 1] += part[:, share:]

            @pl.when(c % np_ == z)
            def _():
                total = own[c]
                mat[...] += exact(total, total.astype(bf16).astype(f32))

        return carry

    lax.fori_loop(0, chunks + LAG * (np_ - 1), step, 0)

    other = chip * 2 + 1 - core
    pending = []
    product = gram[...] + 2.0 * mat[...]
    mine = own_trial()
    squares = as_row(jnp.sum(mine * mine, axis=1, keepdims=True))
    h = vecs // 2
    m1_out[0:h] = jnp.concatenate([product[:h], product[h:]], axis=1)
    m1_out[h:] = jnp.broadcast_to(jnp.concatenate([squares, squares], axis=1), (8, 2 * vecs))
    m1_copy = remote(m1_out, m1_in, m1_s, m1_r, z, other)
    m1_copy.start()
    pending.append(m1_copy)

    b1 = []
    for d in range(chips):
        j = (chip + 1 + d) % chips
        b1_out[d] = acc[2 * j + 1 - core].astype(bf16)
        copy = remote(b1_out.at[d], b1_in.at[d], b1_s.at[d], b1_r.at[d], z, other)
        copy.start()
        b1.append(copy)
        pending.append(copy)
    m1_copy.wait_recv()
    m2[chip] = m1_out[...] + m1_in[...]
    for d in range(1, chips):
        copy = remote(m2.at[chip], m2.at[chip], m2_s.at[d], m2_r.at[chip], z, ((chip + d) % chips) * 2 + core)
        copy.start()
        pending.append(copy)
    for d in range(chips - 1):
        j = (chip + 1 + d) % chips
        b1[d].wait_recv()
        b2_out[d] = (acc[2 * j + core] + b1_in[d].astype(f32)).astype(bf16)
        copy = remote(b2_out.at[d], b2_in.at[d], b2_s.at[d], b2_r.at[d], z, 2 * j + core)
        copy.start()
        pending.append(copy)
    b1[chips - 1].wait_recv()
    coupled = acc[a] + b1_in[chips - 1].astype(f32)

    for d in range(1, chips):
        j = (chip + d) % chips
        remote(m2.at[j], m2.at[j], m2_s.at[d], m2_r.at[j], z, a).wait_recv()
    total = m2[0]
    for j in range(1, chips):
        total = total + m2[j]
    m3[z] = total
    for d in range(1, np_):
        copy = remote(m3.at[z], m3.at[z], m3_s.at[d], m3_r.at[z], (z + d) % np_, a)
        copy.start()
        pending.append(copy)

    for d in range(chips - 1):
        remote(b2_out.at[d], b2_in.at[d], b2_s.at[d], b2_r.at[d], z, a).wait_recv()
        coupled = coupled + b2_in[d].astype(f32)
    mine = own_trial()
    values = own_gaps() * mine + 2.0 * coupled
    sigma[...] = values
    lane = lax.broadcasted_iota(jnp.int32, (vecs, 128), 1)
    sums = jnp.where(
        lane == 0,
        jnp.sum(values * values, axis=1, keepdims=True),
        jnp.where(lane == 1, jnp.sum(values * mine, axis=1, keepdims=True), 0.0),
    )
    n1[a] = jnp.transpose(sums)[:8]
    for d in range(1, na):
        copy = remote(n1.at[a], n1.at[a], n1_s.at[d], n1_r.at[a], z, (a + d) % na)
        copy.start()
        pending.append(copy)
    for d in range(1, na):
        j = (a + d) % na
        remote(n1.at[j], n1.at[j], n1_s.at[d], n1_r.at[j], z, j).wait_recv()
    sums = n1[0]
    for j in range(1, na):
        sums = sums + n1[j]
    n2[z] = sums
    for d in range(1, np_):
        copy = remote(n2.at[z], n2.at[z], n2_s.at[d], n2_r.at[z], (z + d) % np_, a)
        copy.start()
        pending.append(copy)

    for d in range(1, np_):
        j = (z + d) % np_
        remote(m3.at[j], m3.at[j], m3_s.at[d], m3_r.at[j], j, a).wait_recv()
    total = m3[0]
    for j in range(1, np_):
        total = total + m3[j]
    pairs = float(np_ * na * share)
    subspace = jnp.concatenate([total[:h, :vecs], total[:h, vecs:]], axis=0) / pairs
    sub[...] = subspace
    squares = total[h:h + 1, :vecs]
    diagonal = jnp.sum(jnp.where(eye, subspace, 0.0), axis=0, keepdims=True)
    rayleigh = diagonal / (squares / pairs + epsilon)
    column = jnp.sum(jnp.where(eye, rayleigh, 0.0), axis=1, keepdims=True)
    res[...] = sigma[...] - own_trial() * column

    for d in range(1, np_):
        j = (z + d) % np_
        remote(n2.at[j], n2.at[j], n2_s.at[d], n2_r.at[j], j, a).wait_recv()
    sums = n2[0]
    for j in range(1, np_):
        sums = sums + n2[j]
    residual_sq = sums[0:1] - 2.0 * rayleigh * sums[1:2] + rayleigh * rayleigh * squares
    norm[...] = jnp.sqrt(residual_sq / pairs + epsilon)

    @pl.when(after > 0)
    def _():
        for c in range(chunks):
            prefix(c).wait_send()

    @pl.when(z > 0)
    def _():
        for c in range(chunks):
            suffix(c).wait_send()

    for copy in pending:
        copy.wait_send()


def store_kernel(*refs):
    done = refs[8]
    copies = [pltpu.make_async_copy(refs[i], refs[i + 4], done.at[i]) for i in range(4)]
    for copy in copies:
        copy.start()
    for copy in copies:
        copy.wait()


def solution(mesh):
    np_, na = mesh.shape["pair"], mesh.shape["aux"]
    chips = na // 2

    def local(integrals, energy_gaps, trial_vectors):
        rows, cols = integrals.shape
        vecs = trial_vectors.shape[1]
        width = WIDTH
        chunks, share = cols // width, rows // na
        anywhere = pl.BlockSpec(memory_space=pl.ANY)
        dma = pltpu.SemaphoreType.DMA
        message = (vecs // 2 + 8, 2 * vecs)
        results = pl.pallas_call(
            functools.partial(kernel, np_, na, chunks, width, share),
            out_shape=[
                jax.ShapeDtypeStruct((vecs, share), f32),
                jax.ShapeDtypeStruct((vecs, vecs), f32),
                jax.ShapeDtypeStruct((vecs, share), f32),
                jax.ShapeDtypeStruct((1, vecs), f32),
            ],
            in_specs=[pl.BlockSpec(memory_space=pltpu.HBM)] * 3,
            out_specs=[pl.BlockSpec(memory_space=pltpu.VMEM)] * 4,
            scratch_shapes=[
                pltpu.VMEM((chunks, rows, width), bf16),
                pltpu.VMEM((rows // 128, 128), f32),
                pltpu.VMEM((vecs, rows), f32),
                pltpu.VMEM((vecs, rows), bf16),
                pltpu.VMEM((chunks, vecs, width), f32),
                pltpu.VMEM((na, vecs, share), f32),
                pltpu.VMEM((vecs, vecs), f32),
                pltpu.VMEM((vecs, vecs), f32),
                *[pltpu.VMEM((chunks, vecs, width), bf16)] * 4,
                *[pltpu.VMEM((chips, vecs, share), bf16)] * 4,
                pltpu.VMEM(message, f32),
                pltpu.VMEM(message, f32),
                pltpu.VMEM((chips,) + message, f32),
                pltpu.VMEM((np_,) + message, f32),
                pltpu.VMEM((na, 8, vecs), f32),
                pltpu.VMEM((np_, 8, vecs), f32),
                dma((chunks,)), dma((2,)),
                dma((chunks,)), dma((chunks,)), dma((chunks,)), dma((chunks,)),
                dma((chips,)), dma((chips,)), dma((chips,)), dma((chips,)),
                dma, dma, dma((chips,)), dma((chips,)),
                dma((np_,)), dma((np_,)), dma((na,)), dma((na,)), dma((np_,)), dma((np_,)),
            ],
            compiler_params=pltpu.CompilerParams(
                collective_id=0, has_side_effects=True, vmem_limit_bytes=VMEM
            ),
            name="sigma_build",
        )(*[pltpu.with_memory_space_constraint(x, pltpu.HBM) for x in (integrals, energy_gaps.reshape(rows // 128, 128), trial_vectors.T)])
        sigma, subspace, residuals, norms = pl.pallas_call(
            store_kernel,
            out_shape=[jax.ShapeDtypeStruct(x.shape, x.dtype) for x in results],
            in_specs=[pl.BlockSpec(memory_space=pltpu.VMEM)] * 4,
            out_specs=[anywhere] * 4,
            scratch_shapes=[dma((4,))],
            compiler_params=pltpu.CompilerParams(vmem_limit_bytes=VMEM),
            name="store",
        )(*results)
        return sigma.T, subspace, residuals.T, norms.reshape(vecs)

    return jax.shard_map(
        local,
        mesh=mesh,
        in_specs=(P("pair", "aux"), P("pair"), P("pair", None)),
        out_specs=(P(("pair", "aux"), None), P(), P(("pair", "aux"), None), P()),
        check_vma=False,
    )
```

```python
import functools

import jax
import jax.numpy as jnp
from jax import lax
from jax.experimental import pallas as pl
from jax.experimental.pallas import tpu as pltpu
from jax.sharding import PartitionSpec as P

epsilon = 1e-06
MESH = pl.DeviceIdType.MESH
f32, bf16 = jnp.float32, jnp.bfloat16
LANES = 128
VMEM = 48 * 1024 * 1024
LAG = 8
HOLD = 0
FIRST = 0
AHEAD = 3
NT = (((1,), (1,)), ((), ()))


def exact(a, b):
    return lax.dot_general(a, b, NT, precision=lax.Precision.HIGHEST, preferred_element_type=f32)


def kernel(
    np_, na, pieces, share,
    ints_hbm, gaps_hbm, trial_hbm,
    sigma, sub, res, norm,
    ints, gaps, trial, half, own, acc, mat,
    pre_in, pre_out, suf_in, suf_out,
    b1_out, b1_in, b2_out, b2_in,
    g_out, g_in, g3, m1_out, m1_in, m2, sums,
    load, aload, pre_s, pre_r, suf_s, suf_r,
    b1_s, b1_r, b2_s, b2_r, g_s, g_r, g3_s, g3_r, m1_s, m1_r, m2_s, m2_r, n_s, n_r,
):
    z, a = lax.axis_index("pair"), lax.axis_index("aux")
    core, chip, chips = a % 2, a // 2, na // 2
    vecs = trial.shape[0]
    h = vecs // 2
    chunks = pieces // 2
    devices = np_ * na
    me = z * na + a
    other = chip * 2 + 1 - core

    trial_load = pltpu.make_async_copy(trial_hbm, trial, aload.at[0])
    gaps_load = pltpu.make_async_copy(gaps_hbm, gaps, aload.at[1])
    trial_load.start()

    def piece_load(q):
        columns = pl.ds(pl.multiple_of(q * LANES, LANES), LANES)
        return pltpu.make_async_copy(ints_hbm.at[:, columns], ints.at[q], load.at[q])

    for q in range(2 * AHEAD):
        piece_load(q).start()
    gaps_load.start()

    barrier = pltpu.get_barrier_semaphore()
    after = np_ - 1 - z
    bits = [b for b in range(10) if 2 ** b < chips]

    def flip(b):
        return (chip + 2 ** b * (1 - 2 * (chip // 2 ** b % 2))) * 2 + core

    circle = [other] + [flip(b) for b in bits]

    def greet(pair, aux):
        pl.semaphore_signal(barrier, inc=1, device_id={"pair": pair, "aux": aux}, device_id_type=MESH)

    @pl.when(z > 0)
    def _():
        greet(z - 1, a)

    @pl.when(after > 0)
    def _():
        greet(z + 1, a)

    for aux in circle:
        greet(z, aux)

    def remote(src, dst, s, r, pair, aux):
        return pltpu.make_async_remote_copy(
            src_ref=src, dst_ref=dst, send_sem=s, recv_sem=r,
            device_id={"pair": pair, "aux": aux}, device_id_type=MESH,
        )

    def prefix(q):
        return remote(pre_out.at[q], pre_in.at[q], pre_s.at[q], pre_r.at[q], z + 1, a)

    def suffix(q):
        return remote(suf_out.at[q], suf_in.at[q], suf_s.at[q], suf_r.at[q], z - 1, a)

    first = pl.multiple_of(a * share, LANES)
    rows = share // LANES

    def own_trial():
        return trial[:, pl.ds(first, share)]

    def own_gaps():
        return jnp.concatenate([gaps[pl.ds(a * rows + q, 1), :] for q in range(rows)], axis=1)

    eye = lax.broadcasted_iota(jnp.int32, (vecs, vecs), 0) == lax.broadcasted_iota(jnp.int32, (vecs, vecs), 1)

    def as_row(column):
        return jnp.sum(jnp.where(eye, column, 0.0), axis=0, keepdims=True)

    acc[...] = jnp.zeros_like(acc)
    mat[...] = jnp.zeros_like(mat)
    trial_load.wait()
    half[...] = trial[...].astype(bf16)
    gaps_load.wait()
    mine = own_trial()
    gram = exact(mine, mine * own_gaps())
    squares = as_row(jnp.sum(mine * mine, axis=1, keepdims=True))
    g_out[0, 0:h] = jnp.concatenate([gram[:h], gram[h:]], axis=1)
    g_out[0, h:] = jnp.broadcast_to(jnp.concatenate([squares, squares], axis=1), (8, 2 * vecs))
    g_copies = [
        remote(g_out.at[i], g_in.at[i], g_s.at[i], g_r.at[i], z, aux) for i, aux in enumerate(circle)
    ]

    def g_next(i):
        g_copies[i - 1].wait_recv()
        g_out[i] = g_out[i - 1] + g_in[i - 1]
        g_copies[i].start()

    longest = jnp.maximum(z, after)
    inner = (z > 0) & (after > 0)
    hold = FIRST + core * HOLD

    def first_pass(c, carry):
        for k in range(2):
            piece_load(2 * c + k).wait()

        @pl.when(c + AHEAD < chunks)
        def _():
            for k in range(2):
                piece_load(2 * (c + AHEAD) + k).start()

        block = jnp.concatenate([ints[2 * c], ints[2 * c + 1]], axis=1)
        product = jnp.dot(half[...], block, preferred_element_type=f32)
        own[2 * c] = product[:, :LANES]
        own[2 * c + 1] = product[:, LANES:]

        @pl.when(c == FIRST)
        def _():
            pl.semaphore_wait(barrier, len(circle) + jnp.where(inner, 2, 1))
            g_copies[0].start()

        @pl.when(z == 0)
        def _():
            pre_out[2 * c] = own[2 * c].astype(bf16)
            pre_out[2 * c + 1] = own[2 * c + 1].astype(bf16)

        @pl.when(after == 0)
        def _():
            suf_out[2 * c] = own[2 * c].astype(bf16)
            suf_out[2 * c + 1] = own[2 * c + 1].astype(bf16)

        def send(b):
            @pl.when(z == 0)
            def _():
                prefix(2 * b).start()
                prefix(2 * b + 1).start()

            @pl.when(after == 0)
            def _():
                suffix(2 * b).start()
                suffix(2 * b + 1).start()

        @pl.when(c == hold)
        def _():
            lax.fori_loop(0, hold, lambda b, x: (send(b), x)[1], 0)

        @pl.when(c >= hold)
        def _():
            send(c)

        return carry

    lax.fori_loop(0, chunks, first_pass, 0)
    for i in range(1, min(2, len(circle))):
        g_next(i)
    base = jnp.where(inner, jnp.minimum(z, after), longest)

    def second_pass(q):
        total = own[q]
        aux = total.astype(bf16)
        low = (total - aux.astype(f32)).astype(bf16)
        return aux, lax.dot_general(
            jnp.concatenate([aux, low], axis=0), aux, NT, preferred_element_type=f32
        )

    def step(t, carry):
        p = t - LAG * (z - base)

        @pl.when((p >= 0) & (p < pieces) & inner)
        def _():
            prefix(p).wait_recv()
            pre_out[p] = (own[p] + pre_in[p].astype(f32)).astype(bf16)
            prefix(p).start()

        s = t - LAG * (after - base)

        @pl.when((s >= 0) & (s < pieces) & inner)
        def _():
            suffix(s).wait_recv()
            suf_out[s] = (own[s] + suf_in[s].astype(f32)).astype(bf16)
            suffix(s).start()

        q = t - LAG * (longest - base)

        @pl.when(q >= 0)
        def _():
            @pl.when(after == 0)
            def _():
                prefix(q).wait_recv()

            @pl.when(z == 0)
            def _():
                suffix(q).wait_recv()

            @pl.when(z > 0)
            def _():
                own[q] = own[q] + pre_in[q].astype(f32)

            @pl.when(after > 0)
            def _():
                own[q] = own[q] + suf_in[q].astype(f32)

            @pl.when(q < pieces - 1)
            def _():
                aux, square = second_pass(q)
                mat[...] += square
                for b in range(chips):
                    part = lax.dot_general(
                        aux, ints[q, pl.ds(b * 2 * share, 2 * share), :], NT, preferred_element_type=f32
                    )
                    acc[2 * b] += part[:, :share]
                    acc[2 * b + 1] += part[:, share:]

        @pl.when(t == jnp.where(inner, LAG - 1, 0))
        def _():
            for i in range(2, len(circle)):
                g_next(i)

        return carry

    lax.fori_loop(0, pieces + LAG * (longest - base), step, 0)

    pending = list(g_copies)
    g_copies[-1].wait_recv()
    aux, square = second_pass(pieces - 1)

    def chip_at(d):
        return (chip + jnp.where(chip % 2 == 1, d, chips - d)) % chips

    def last_part(i):
        return lax.dot_general(
            aux, ints[pieces - 1, pl.ds(pl.multiple_of(i * share, LANES), share), :], NT,
            preferred_element_type=f32,
        )

    b1 = []
    for d in range(1, chips + 1):
        i = 2 * chip_at(d) + 1 - core
        b1_out[d - 1] = (acc[i] + last_part(i)).astype(bf16)
        copy = remote(b1_out.at[d - 1], b1_in.at[d - 1], b1_s.at[d - 1], b1_r.at[d - 1], z, other)
        copy.start()
        b1.append(copy)
        pending.append(copy)
    for d in range(1, chips + 1):
        i = 2 * chip_at(d) + core
        acc[i] += last_part(i)
    square = mat[...] + square
    square = square[:vecs] + square[vecs:]
    m1_out[...] = jnp.concatenate([square[:h], square[h:]], axis=1)
    m1_copy = remote(m1_out, m1_in, m1_s, m1_r, z, other)
    m1_copy.start()
    pending.append(m1_copy)
    for d in range(1, chips):
        j = chip_at(d)
        b1[d - 1].wait_recv()
        b2_out[d - 1] = (acc[2 * j + core] + b1_in[d - 1].astype(f32)).astype(bf16)
        copy = remote(b2_out.at[d - 1], b2_in.at[d - 1], b2_s.at[d - 1], b2_r.at[d - 1], z, 2 * j + core)
        copy.start()
        pending.append(copy)
    b1[chips - 1].wait_recv()
    coupled = acc[a] + b1_in[chips - 1].astype(f32)

    g3[z] = g_out[len(circle) - 1] + g_in[len(circle) - 1]
    for d in range(1, np_):
        copy = remote(g3.at[z], g3.at[z], g3_s.at[d], g3_r.at[z], (z + d) % np_, a)
        copy.start()
        pending.append(copy)
    m1_copy.wait_recv()
    m2[chip] = m1_out[...] + m1_in[...]
    for d in range(1, chips):
        copy = remote(m2.at[chip], m2.at[chip], m2_s.at[d], m2_r.at[chip], z, ((chip + d) % chips) * 2 + core)
        copy.start()
        pending.append(copy)

    for d in range(1, chips):
        remote(b2_out.at[d - 1], b2_in.at[d - 1], b2_s.at[d - 1], b2_r.at[d - 1], z, a).wait_recv()
        coupled = coupled + b2_in[d - 1].astype(f32)
    mine = own_trial()
    values = own_gaps() * mine + 2.0 * coupled
    both = jnp.concatenate([values * values, values * mine], axis=0)
    folded = both[:, :LANES]
    for q in range(1, rows):
        folded = folded + both[:, q * LANES:(q + 1) * LANES]
    sums[me] = jnp.sum(jnp.transpose(folded), axis=0, keepdims=True)

    def tell(pair, aux):
        remote(sums.at[me], sums.at[me], n_s, n_r, pair, aux).start()

    def tell_plane(i, carry):
        pair = jnp.where(2 * z < np_, np_ - 1 - i, i)
        for d in range(1, na):
            tell(pair, (a + d) % na)

        @pl.when(pair != z)
        def _():
            tell(pair, a)

        return carry

    lax.fori_loop(0, np_, tell_plane, 0)
    sigma[...] = values

    for d in range(1, chips):
        j = (chip + d) % chips
        remote(m2.at[j], m2.at[j], m2_s.at[d], m2_r.at[j], z, a).wait_recv()
    square = m2[0]
    for j in range(1, chips):
        square = square + m2[j]
    for d in range(1, np_):
        j = (z + d) % np_
        remote(g3.at[j], g3.at[j], g3_s.at[d], g3_r.at[j], j, a).wait_recv()
    total = g3[0]
    for j in range(1, np_):
        total = total + g3[j]
    pairs = float(devices * share)
    packed = total[:h] + 2.0 * square
    subspace = jnp.concatenate([packed[:, :vecs], packed[:, vecs:]], axis=0) / pairs
    sub[...] = subspace
    squares = total[h:h + 1, :vecs]
    diagonal = jnp.sum(jnp.where(eye, subspace, 0.0), axis=0, keepdims=True)
    rayleigh = diagonal / (squares / pairs + epsilon)
    column = jnp.sum(jnp.where(eye, rayleigh, 0.0), axis=1, keepdims=True)
    res[...] = sigma[...] - own_trial() * column

    everyone = remote(sums.at[pl.ds(0, devices - 1)], sums.at[pl.ds(0, devices - 1)], n_s, n_r, z, other)
    everyone.wait_recv()
    both = jnp.sum(sums[...], axis=0)
    residual_sq = both[:, :vecs] - 2.0 * rayleigh * both[:, vecs:] + rayleigh * rayleigh * squares
    norm[...] = jnp.sqrt(residual_sq / pairs + epsilon)

    @pl.when(after > 0)
    def _():
        for q in range(pieces):
            prefix(q).wait_send()

    @pl.when(z > 0)
    def _():
        for q in range(pieces):
            suffix(q).wait_send()

    for copy in pending:
        copy.wait_send()
    everyone.wait_send()


def store_kernel(*refs):
    done = refs[8]
    copies = [pltpu.make_async_copy(refs[i], refs[i + 4], done.at[i]) for i in range(4)]
    for copy in copies:
        copy.start()
    for copy in copies:
        copy.wait()


def solution(mesh):
    np_, na = mesh.shape["pair"], mesh.shape["aux"]
    chips = na // 2

    def local(integrals, energy_gaps, trial_vectors):
        rows, cols = integrals.shape
        vecs = trial_vectors.shape[1]
        pieces, share = cols // LANES, rows // na
        anywhere = pl.BlockSpec(memory_space=pl.ANY)
        local_block = pl.BlockSpec(memory_space=pltpu.VMEM)
        dma = pltpu.SemaphoreType.DMA
        stages = 1 + (chips - 1).bit_length()
        message = (vecs // 2 + 8, 2 * vecs)
        matrix = (vecs // 2, 2 * vecs)
        inputs = (integrals, energy_gaps.reshape(rows // LANES, LANES), trial_vectors.T)
        results = pl.pallas_call(
            functools.partial(kernel, np_, na, pieces, share),
            out_shape=[
                jax.ShapeDtypeStruct((vecs, share), f32),
                jax.ShapeDtypeStruct((vecs, vecs), f32),
                jax.ShapeDtypeStruct((vecs, share), f32),
                jax.ShapeDtypeStruct((1, vecs), f32),
            ],
            in_specs=[anywhere] * 3,
            out_specs=[local_block] * 4,
            scratch_shapes=[
                pltpu.VMEM((pieces, rows, LANES), bf16),
                pltpu.VMEM((rows // LANES, LANES), f32),
                pltpu.VMEM((vecs, rows), f32),
                pltpu.VMEM((vecs, rows), bf16),
                pltpu.VMEM((pieces, vecs, LANES), f32),
                pltpu.VMEM((na, vecs, share), f32),
                pltpu.VMEM((2 * vecs, vecs), f32),
                *[pltpu.VMEM((pieces, vecs, LANES), bf16)] * 4,
                *[pltpu.VMEM((chips, vecs, share), bf16)] * 4,
                pltpu.VMEM((stages,) + message, f32),
                pltpu.VMEM((stages,) + message, f32),
                pltpu.VMEM((np_,) + message, f32),
                pltpu.VMEM(matrix, f32),
                pltpu.VMEM(matrix, f32),
                pltpu.VMEM((chips,) + matrix, f32),
                pltpu.VMEM((np_ * na, 1, 2 * vecs), f32),
                dma((pieces,)), dma((2,)),
                dma((pieces,)), dma((pieces,)), dma((pieces,)), dma((pieces,)),
                dma((chips,)), dma((chips,)), dma((chips,)), dma((chips,)),
                dma((stages,)), dma((stages,)), dma((np_,)), dma((np_,)),
                dma, dma, dma((chips,)), dma((chips,)), dma, dma,
            ],
            compiler_params=pltpu.CompilerParams(
                collective_id=0, has_side_effects=True, vmem_limit_bytes=VMEM
            ),
            name="sigma_build",
        )(*[pltpu.with_memory_space_constraint(x, pltpu.HBM) for x in inputs])
        sigma, subspace, residuals, norms = pl.pallas_call(
            store_kernel,
            out_shape=[jax.ShapeDtypeStruct(x.shape, x.dtype) for x in results],
            in_specs=[local_block] * 4,
            out_specs=[anywhere] * 4,
            scratch_shapes=[dma((4,))],
            compiler_params=pltpu.CompilerParams(vmem_limit_bytes=VMEM),
            name="store",
        )(*results)
        return sigma.T, subspace, residuals.T, norms.reshape(vecs)

    return jax.shard_map(
        local,
        mesh=mesh,
        in_specs=(P("pair", "aux"), P("pair"), P("pair", None)),
        out_specs=(P(("pair", "aux"), None), P(), P(("pair", "aux"), None), P()),
        check_vma=False,
    )
```

```python
import functools

import jax
import jax.numpy as jnp
from jax import lax
from jax.experimental import pallas as pl
from jax.experimental.pallas import tpu as pltpu
from jax.sharding import PartitionSpec as P

epsilon = 1e-06
MESH = pl.DeviceIdType.MESH
f32, bf16 = jnp.float32, jnp.bfloat16
LANES = 128
VMEM = 48 * 1024 * 1024
WIDTH = 2 * LANES
AHEAD = 3
NT = (((1,), (1,)), ((), ()))


def exact(a, b):
    return lax.dot_general(a, b, NT, precision=lax.Precision.HIGHEST, preferred_element_type=f32)


def kernel(
    np_, na, chunks, share,
    ints_hbm, gaps_hbm, trial_hbm,
    sigma, sub, res, norm,
    ints, gaps, trial, half, own, acc, mat,
    c_in, c_out, j_in,
    b1_out, b1_in, b2_out, b2_in,
    g_out, g_in, g3, m1_out, m1_in, m2, sums,
    load, aload, c_s, c_r, j_s, j_r,
    b1_s, b1_r, b2_s, b2_r, g_s, g_r, g3_s, g3_r, m1_s, m1_r, m2_s, m2_r, n_s, n_r,
):
    z, a = lax.axis_index("pair"), lax.axis_index("aux")
    core, chip, chips = a % 2, a // 2, na // 2
    vecs = trial.shape[0]
    h = vecs // 2
    devices = np_ * na
    me = z * na + a
    other = chip * 2 + 1 - core

    trial_load = pltpu.make_async_copy(trial_hbm, trial, aload.at[0])
    gaps_load = pltpu.make_async_copy(gaps_hbm, gaps, aload.at[1])
    trial_load.start()

    def chunk_load(c):
        columns = pl.ds(pl.multiple_of(c * WIDTH, WIDTH), WIDTH)
        return pltpu.make_async_copy(ints_hbm.at[:, columns], ints.at[c], load.at[c])

    for c in range(min(AHEAD, chunks)):
        chunk_load(c).start()
    gaps_load.start()

    barrier = pltpu.get_barrier_semaphore()
    after = np_ - 1 - z
    bits = [b for b in range(10) if 2 ** b < chips]

    def flip(b):
        return (chip + 2 ** b * (1 - 2 * (chip // 2 ** b % 2))) * 2 + core

    circle = [other] + [flip(b) for b in bits]

    def greet(pair, aux):
        pl.semaphore_signal(barrier, inc=1, device_id={"pair": pair, "aux": aux}, device_id_type=MESH)

    @pl.when(z > 0)
    def _():
        greet(z - 1, a)

    @pl.when(after > 0)
    def _():
        greet(z + 1, a)

    for aux in circle:
        greet(z, aux)

    inner = (z > 0) & (after > 0)
    near = jnp.where(z < after, 0, 1)
    late = core == 0 if np_ == 4 else core < 0

    @pl.when(jnp.logical_not(inner) & late)
    def _():
        greet(z + 2 - 4 * near, a)

    def remote(src, dst, s, r, pair, aux):
        return pltpu.make_async_remote_copy(
            src_ref=src, dst_ref=dst, send_sem=s, recv_sem=r,
            device_id={"pair": pair, "aux": aux}, device_id_type=MESH,
        )

    def chain(k, c):
        return remote(c_out.at[k, c], c_in.at[k, c], c_s.at[k, c], c_r.at[k, c], z + 1 - 2 * k, a)

    def jump(c):
        return remote(c_out.at[near, c], j_in.at[c], j_s.at[c], j_r.at[c], z + 2 - 4 * near, a)

    cut = jnp.where(late, 0, chunks)
    first = pl.multiple_of(a * share, LANES)
    rows = share // LANES

    def own_trial():
        return trial[:, pl.ds(first, share)]

    def own_gaps():
        return jnp.concatenate([gaps[pl.ds(a * rows + q, 1), :] for q in range(rows)], axis=1)

    eye = lax.broadcasted_iota(jnp.int32, (vecs, vecs), 0) == lax.broadcasted_iota(jnp.int32, (vecs, vecs), 1)

    def as_row(column):
        return jnp.sum(jnp.where(eye, column, 0.0), axis=0, keepdims=True)

    acc[...] = jnp.zeros_like(acc)
    mat[...] = jnp.zeros_like(mat)
    trial_load.wait()
    half[...] = trial[...].astype(bf16)
    gaps_load.wait()
    mine = own_trial()
    gram = exact(mine, mine * own_gaps())
    squares = as_row(jnp.sum(mine * mine, axis=1, keepdims=True))
    g_out[0, 0:h] = jnp.concatenate([gram[:h], gram[h:]], axis=1)
    g_out[0, h:] = jnp.broadcast_to(jnp.concatenate([squares, squares], axis=1), (8, 2 * vecs))
    g_copies = [
        remote(g_out.at[i], g_in.at[i], g_s.at[i], g_r.at[i], z, aux) for i, aux in enumerate(circle)
    ]

    def g_next(i):
        g_copies[i - 1].wait_recv()
        g_out[i] = g_out[i - 1] + g_in[i - 1]
        g_copies[i].start()

    def first_pass(c, carry):
        chunk_load(c).wait()

        @pl.when(c + AHEAD < chunks)
        def _():
            chunk_load(c + AHEAD).start()

        product = jnp.dot(half[...], ints[c], preferred_element_type=f32)
        own[c] = product

        @pl.when(c == 0)
        def _():
            pl.semaphore_wait(barrier, len(circle) + jnp.where(inner, jnp.where(late, 3, 2), 1))
            g_copies[0].start()

        @pl.when(jnp.logical_not(inner))
        def _():
            c_out[near, c] = product.astype(bf16)
            chain(near, c).start()

        @pl.when(inner & (c >= cut))
        def _():
            c_out[1 - near, c] = product.astype(bf16)
            chain(1 - near, c).start()

        return carry

    lax.fori_loop(0, chunks, first_pass, 0)
    for i in range(1, min(2, len(circle))):
        g_next(i)

    def forward(k, c):
        chain(k, c).wait_recv()
        c_out[k, c] = (own[c] + c_in[k, c].astype(f32)).astype(bf16)
        chain(k, c).start()

    def near_step(c, carry):
        forward(near, c)

        @pl.when(c >= cut)
        def _():
            jump(c).start()

        return carry

    def far_step(c, carry):
        forward(1 - near, c)
        return carry

    @pl.when(inner)
    def _():
        lax.fori_loop(0, chunks, near_step, 0)

    for i in range(2, len(circle)):
        g_next(i)

    @pl.when(inner)
    def _():
        lax.fori_loop(0, cut, far_step, 0)

    def total_of(c):
        @pl.when(jnp.logical_not(inner) | (c >= cut))
        def _():
            chain(1 - near, c).wait_recv()

        own[c] = own[c] + c_in[1 - near, c].astype(f32)

        @pl.when(inner)
        def _():
            own[c] = own[c] + c_in[near, c].astype(f32)

        @pl.when(jnp.logical_not(inner) & (c >= cut))
        def _():
            jump(c).wait_recv()
            own[c] = own[c] + j_in[c].astype(f32)

        total = own[c]
        aux = total.astype(bf16)
        low = (total - aux.astype(f32)).astype(bf16)
        return aux, lax.dot_general(
            jnp.concatenate([aux, low], axis=0), aux, NT, preferred_element_type=f32
        )

    def second_pass(i, carry):
        c = (i + cut) % chunks
        aux, square = total_of(c)
        mat[...] += square
        for b in range(chips):
            part = lax.dot_general(
                aux, ints[c, pl.ds(b * 2 * share, 2 * share), :], NT, preferred_element_type=f32
            )
            acc[2 * b] += part[:, :share]
            acc[2 * b + 1] += part[:, share:]
        return carry

    lax.fori_loop(0, chunks - 1, second_pass, 0)

    pending = list(g_copies)
    g_copies[-1].wait_recv()
    last = (chunks - 1 + cut) % chunks
    aux, square = total_of(last)

    def chip_at(d):
        return (chip + jnp.where(chip % 2 == 1, d, chips - d)) % chips

    def last_part(i):
        return lax.dot_general(
            aux, ints[last, pl.ds(pl.multiple_of(i * share, LANES), share), :], NT,
            preferred_element_type=f32,
        )

    b1 = []
    for d in range(1, chips + 1):
        i = 2 * chip_at(d) + 1 - core
        b1_out[d - 1] = (acc[i] + last_part(i)).astype(bf16)
        copy = remote(b1_out.at[d - 1], b1_in.at[d - 1], b1_s.at[d - 1], b1_r.at[d - 1], z, other)
        copy.start()
        b1.append(copy)
        pending.append(copy)
    for d in range(1, chips + 1):
        i = 2 * chip_at(d) + core
        acc[i] += last_part(i)
    square = mat[...] + square
    square = square[:vecs] + square[vecs:]
    m1_out[...] = jnp.concatenate([square[:h], square[h:]], axis=1)
    m1_copy = remote(m1_out, m1_in, m1_s, m1_r, z, other)
    m1_copy.start()
    pending.append(m1_copy)
    for d in range(1, chips):
        j = chip_at(d)
        b1[d - 1].wait_recv()
        b2_out[d - 1] = (acc[2 * j + core] + b1_in[d - 1].astype(f32)).astype(bf16)
        copy = remote(b2_out.at[d - 1], b2_in.at[d - 1], b2_s.at[d - 1], b2_r.at[d - 1], z, 2 * j + core)
        copy.start()
        pending.append(copy)
    b1[chips - 1].wait_recv()
    coupled = acc[a] + b1_in[chips - 1].astype(f32)

    g3[z] = g_out[len(circle) - 1] + g_in[len(circle) - 1]
    for d in range(1, np_):
        copy = remote(g3.at[z], g3.at[z], g3_s.at[d], g3_r.at[z], (z + d) % np_, a)
        copy.start()
        pending.append(copy)
    m1_copy.wait_recv()
    m2[chip] = m1_out[...] + m1_in[...]
    for d in range(1, chips):
        copy = remote(m2.at[chip], m2.at[chip], m2_s.at[d], m2_r.at[chip], z, ((chip + d) % chips) * 2 + core)
        copy.start()
        pending.append(copy)

    for d in range(1, chips):
        remote(b2_out.at[d - 1], b2_in.at[d - 1], b2_s.at[d - 1], b2_r.at[d - 1], z, a).wait_recv()
        coupled = coupled + b2_in[d - 1].astype(f32)
    mine = own_trial()
    values = own_gaps() * mine + 2.0 * coupled
    both = jnp.concatenate([values * values, values * mine], axis=0)
    folded = both[:, :LANES]
    for q in range(1, rows):
        folded = folded + both[:, q * LANES:(q + 1) * LANES]
    sums[me] = jnp.sum(jnp.transpose(folded), axis=0, keepdims=True)

    def tell(pair, aux):
        remote(sums.at[me], sums.at[me], n_s, n_r, pair, aux).start()

    def tell_plane(i, carry):
        pair = jnp.where(2 * z < np_, np_ - 1 - i, i)
        for d in range(1, na):
            tell(pair, (a + d) % na)

        @pl.when(pair != z)
        def _():
            tell(pair, a)

        return carry

    lax.fori_loop(0, np_, tell_plane, 0)
    sigma[...] = values

    for d in range(1, chips):
        j = (chip + d) % chips
        remote(m2.at[j], m2.at[j], m2_s.at[d], m2_r.at[j], z, a).wait_recv()
    square = m2[0]
    for j in range(1, chips):
        square = square + m2[j]
    for d in range(1, np_):
        j = (z + d) % np_
        remote(g3.at[j], g3.at[j], g3_s.at[d], g3_r.at[j], j, a).wait_recv()
    total = g3[0]
    for j in range(1, np_):
        total = total + g3[j]
    pairs = float(devices * share)
    packed = total[:h] + 2.0 * square
    subspace = jnp.concatenate([packed[:, :vecs], packed[:, vecs:]], axis=0) / pairs
    sub[...] = subspace
    squares = total[h:h + 1, :vecs]
    diagonal = jnp.sum(jnp.where(eye, subspace, 0.0), axis=0, keepdims=True)
    rayleigh = diagonal / (squares / pairs + epsilon)
    column = jnp.sum(jnp.where(eye, rayleigh, 0.0), axis=1, keepdims=True)
    res[...] = sigma[...] - own_trial() * column

    everyone = remote(sums.at[pl.ds(0, devices - 1)], sums.at[pl.ds(0, devices - 1)], n_s, n_r, z, other)
    everyone.wait_recv()
    both = jnp.sum(sums[...], axis=0)
    residual_sq = both[:, :vecs] - 2.0 * rayleigh * both[:, vecs:] + rayleigh * rayleigh * squares
    norm[...] = jnp.sqrt(residual_sq / pairs + epsilon)

    @pl.when(after > 0)
    def _():
        for c in range(chunks):
            chain(0, c).wait_send()

    @pl.when(z > 0)
    def _():
        for c in range(chunks):
            chain(1, c).wait_send()

    @pl.when(inner)
    def _():
        lax.fori_loop(cut, chunks, lambda c, x: (jump(c).wait_send(), x)[1], 0)

    for copy in pending:
        copy.wait_send()
    everyone.wait_send()


def store_kernel(*refs):
    done = refs[8]
    copies = [pltpu.make_async_copy(refs[i], refs[i + 4], done.at[i]) for i in range(4)]
    for copy in copies:
        copy.start()
    for copy in copies:
        copy.wait()


def solution(mesh):
    np_, na = mesh.shape["pair"], mesh.shape["aux"]
    chips = na // 2

    def local(integrals, energy_gaps, trial_vectors):
        rows, cols = integrals.shape
        vecs = trial_vectors.shape[1]
        chunks, share = cols // WIDTH, rows // na
        anywhere = pl.BlockSpec(memory_space=pl.ANY)
        local_block = pl.BlockSpec(memory_space=pltpu.VMEM)
        dma = pltpu.SemaphoreType.DMA
        stages = 1 + (chips - 1).bit_length()
        message = (vecs // 2 + 8, 2 * vecs)
        matrix = (vecs // 2, 2 * vecs)
        inputs = (integrals, energy_gaps.reshape(rows // LANES, LANES), trial_vectors.T)
        results = pl.pallas_call(
            functools.partial(kernel, np_, na, chunks, share),
            out_shape=[
                jax.ShapeDtypeStruct((vecs, share), f32),
                jax.ShapeDtypeStruct((vecs, vecs), f32),
                jax.ShapeDtypeStruct((vecs, share), f32),
                jax.ShapeDtypeStruct((1, vecs), f32),
            ],
            in_specs=[anywhere] * 3,
            out_specs=[local_block] * 4,
            scratch_shapes=[
                pltpu.VMEM((chunks, rows, WIDTH), bf16),
                pltpu.VMEM((rows // LANES, LANES), f32),
                pltpu.VMEM((vecs, rows), f32),
                pltpu.VMEM((vecs, rows), bf16),
                pltpu.VMEM((chunks, vecs, WIDTH), f32),
                pltpu.VMEM((na, vecs, share), f32),
                pltpu.VMEM((2 * vecs, vecs), f32),
                *[pltpu.VMEM((2, chunks, vecs, WIDTH), bf16)] * 2,
                pltpu.VMEM((chunks, vecs, WIDTH), bf16),
                *[pltpu.VMEM((chips, vecs, share), bf16)] * 4,
                pltpu.VMEM((stages,) + message, f32),
                pltpu.VMEM((stages,) + message, f32),
                pltpu.VMEM((np_,) + message, f32),
                pltpu.VMEM(matrix, f32),
                pltpu.VMEM(matrix, f32),
                pltpu.VMEM((chips,) + matrix, f32),
                pltpu.VMEM((np_ * na, 1, 2 * vecs), f32),
                dma((chunks,)), dma((2,)),
                dma((2, chunks)), dma((2, chunks)), dma((chunks,)), dma((chunks,)),
                dma((chips,)), dma((chips,)), dma((chips,)), dma((chips,)),
                dma((stages,)), dma((stages,)), dma((np_,)), dma((np_,)),
                dma, dma, dma((chips,)), dma((chips,)), dma, dma,
            ],
            compiler_params=pltpu.CompilerParams(
                collective_id=0, has_side_effects=True, vmem_limit_bytes=VMEM
            ),
            name="sigma_build",
        )(*[pltpu.with_memory_space_constraint(x, pltpu.HBM) for x in inputs])
        sigma, subspace, residuals, norms = pl.pallas_call(
            store_kernel,
            out_shape=[jax.ShapeDtypeStruct(x.shape, x.dtype) for x in results],
            in_specs=[local_block] * 4,
            out_specs=[anywhere] * 4,
            scratch_shapes=[dma((4,))],
            compiler_params=pltpu.CompilerParams(vmem_limit_bytes=VMEM),
            name="store",
        )(*results)
        return sigma.T, subspace, residuals.T, norms.reshape(vecs)

    return jax.shard_map(
        local,
        mesh=mesh,
        in_specs=(P("pair", "aux"), P("pair"), P("pair", None)),
        out_specs=(P(("pair", "aux"), None), P(), P(("pair", "aux"), None), P()),
        check_vma=False,
    )
```
